128 devices in a mesh: gx: 4 (over y_hi, core), gy: 32 (over x, y_lo, z).
Axes of the slice: x: 4, y: 4 (y_hi: 2, y_lo: 2; y = y_hi * 2 + y_lo), z: 4, core: 2. Of those that a mesh axis runs over, the one named last changes fastest.
Arguments:
- tokens: bfloat16 [4, 256, 6144], P('gx', None, 'gy'), may hold values from -6 to 6
- norm_gain: float32 [6144], replicated, may hold values from 0.1 to 1.9
- qkv_weight: bfloat16 [6144, 3, 4096], P('gx', None, 'gy'), may hold values from -0.078125 to 0.078125
- up_weight: bfloat16 [6144, 24576], P('gx', 'gy'), may hold values from -0.078125 to 0.078125
- query_gain: float32 [128], replicated, may hold values from 0.1 to 1.9
- key_gain: float32 [128], replicated, may hold values from 0.1 to 1.9
- out_weight: bfloat16 [4096, 6144], P('gy', 'gx'), may hold values from -0.09375 to 0.09375
- down_weight: bfloat16 [24576, 6144], P('gy', 'gx'), may hold values from -0.0390625 to 0.0390625
- attention_keep: int32 [4, 256, 6144], P('gx', None, 'gy'), may hold values 0 or 1
- feedforward_keep: int32 [4, 256, 6144], P('gx', None, 'gy'), may hold values 0 or 1
Outputs:
- block_out: bfloat16 [4, 256, 6144], P('gx', None, 'gy')
The draws below stay inside these ranges and needn't reach their ends.
All inputs are finite; a program needn't handle non-finite values. No bound on the sum of `attention_keep` or of `feedforward_keep` on one device may be relied on, other than what follows from the above.
Results may differ from the reference program's by a relative error of at most 0.017.
Values may be sent and summed in bfloat16 or wider, within the bound.
A program may use at most 64 MiB of HBM per device.

```python
import jax
import jax.numpy as jnp
from jax import lax

D = 6144
HEADS = 32
HDIM = 128
FF = 24576
SEQ = 256
IMAGES = 4
INNER = 4096
N_GX = 4
N_GY = 32


def place_ends(entries, key, low, top_value):
    longest = entries.shape.index(max(entries.shape))
    spots = []
    for shift in (0, 1):
        where = [jax.random.randint(jax.random.fold_in(key, axis), (), 0, length) for axis, length in enumerate(entries.shape)]
        where[longest] = (where[longest] + shift) % entries.shape[longest]
        spots.append(tuple(where))
    return entries.at[spots[0]].set(low).at[spots[1]].set(top_value)


def steps_of(stream_key, dims, split, low, largest):
    level, own = 1.0, jax.random.fold_in(stream_key, 6)
    for dim, shards_of in split:
        steps = jnp.exp(jax.random.uniform(jax.random.fold_in(own, dim), (shards_of,), jnp.float32, low / len(split), largest / len(split)))
        level = level * jnp.repeat(steps, dims[dim] // shards_of).reshape([-1 if axis == dim else 1 for axis in range(len(dims))])
    return level


def scatter_about(rng, extent, spread, limit, cuts=(), kind=jnp.bfloat16):
    values = spread * jax.random.normal(rng, extent, jnp.float32)
    if cuts:
        values = values * steps_of(rng, extent, cuts, -0.22, 0.18)
    return jnp.clip(values, -limit, limit).astype(kind)


def setup_inputs(seed: int = 0) -> dict:
    key_of = jax.random.split(jax.random.key(seed), 11)
    return {
        "tokens": scatter_about(key_of[0], (IMAGES, SEQ, D), 1.0, 6.0, ((0, 4), (2, 32))),
        "norm_gain": jnp.clip(1.0 + 0.18 * jax.random.normal(key_of[1], (D,), jnp.float32), 0.1, 1.9),
        "qkv_weight": scatter_about(key_of[2], (D, 3, INNER), D ** -0.5, 0.078125, ((0, 4), (2, 32))),
        "up_weight": scatter_about(key_of[3], (D, FF), D ** -0.5, 0.078125, ((0, 4), (1, 32))),
        "query_gain": jnp.clip(1.0 + 0.18 * jax.random.normal(key_of[4], (HDIM,), jnp.float32), 0.1, 1.9),
        "key_gain": jnp.clip(1.0 + 0.18 * jax.random.normal(key_of[5], (HDIM,), jnp.float32), 0.1, 1.9),
        "out_weight": scatter_about(key_of[6], (INNER, D), INNER ** -0.5, 0.09375, ((0, 32), (1, 4))),
        "down_weight": scatter_about(key_of[7], (FF, D), FF ** -0.5, 0.0390625, ((0, 32), (1, 4))),
        "attention_keep": place_ends((jax.random.randint(key_of[8], (IMAGES, SEQ, D), 0, 10) < 9).astype(jnp.int32), jax.random.fold_in(key_of[8], 1), 0, 1),
        "feedforward_keep": place_ends((jax.random.randint(key_of[9], (IMAGES, SEQ, D), 0, 10) < 9).astype(jnp.int32), jax.random.fold_in(key_of[9], 1), 0, 1),
    }


epsilon = 1e-06
keep_scale = 1.0 / 0.9

def layer_norm(values, gain):
    center = values - lax.optimization_barrier(jnp.mean(values, axis=-1, keepdims=True))
    variance = lax.optimization_barrier(jnp.mean(center * center, axis=-1, keepdims=True))
    return center * lax.rsqrt(variance + epsilon) * gain

def head_norm(values, gain):
    row_count = values.shape[0]
    shaped = values.reshape(row_count, -1, gain.shape[0])
    return layer_norm(shaped, gain).reshape(row_count, -1)

def rounded_sum(left, right, block_width, count):

    def accumulate(running, index):
        offset = index * block_width
        segment = lax.dynamic_slice_in_dim(left, offset, block_width, 1)
        rows_part = lax.dynamic_slice_in_dim(right, offset, block_width, 0)
        term = jnp.dot(segment, rows_part, preferred_element_type=jnp.float32).astype(jnp.bfloat16)
        term = lax.optimization_barrier(term)
        return (running + term.astype(jnp.float32), None)
    begin = jnp.zeros((left.shape[0], right.shape[1]), jnp.float32)
    total, unused = lax.scan(accumulate, begin, jnp.arange(count, dtype=jnp.int32))
    return total

def reference(tokens, norm_gain, qkv_weight, up_weight, query_gain, key_gain, out_weight, down_weight, attention_keep, feedforward_keep):
    row_total = IMAGES * SEQ
    inner = HEADS * HDIM
    normed = layer_norm(tokens.astype(jnp.float32), norm_gain).astype(jnp.bfloat16).reshape(row_total, D)
    joined = jnp.concatenate([qkv_weight.reshape(D, 3 * inner), up_weight], axis=1)
    united = rounded_sum(normed, joined, D // N_GX, N_GX)
    queries = head_norm(united[:, :inner], query_gain).astype(jnp.bfloat16)
    keys = head_norm(united[:, inner:2 * inner], key_gain).astype(jnp.bfloat16)
    values = united[:, 2 * inner:3 * inner].astype(jnp.bfloat16)
    query_grid = queries.reshape(IMAGES, SEQ, HEADS, HDIM).astype(jnp.float32)
    key_grid = keys.reshape(IMAGES, SEQ, HEADS, HDIM).astype(jnp.float32)
    value_grid = values.reshape(IMAGES, SEQ, HEADS, HDIM).astype(jnp.float32)
    scores = jnp.einsum('bshd,bthd->bhst', query_grid, key_grid) * HDIM ** (-0.5)
    raised = jnp.exp(scores)
    weights = (raised / lax.optimization_barrier(jnp.sum(raised, axis=-1, keepdims=True))).astype(jnp.bfloat16)
    attended = jnp.einsum('bhst,bthd->bshd', weights.astype(jnp.float32), value_grid)
    attended = attended.astype(jnp.bfloat16).reshape(row_total, inner)
    hidden = jax.nn.gelu(united[:, 3 * inner:], approximate=False).astype(jnp.bfloat16)
    attention_out = rounded_sum(attended, out_weight, inner // N_GY, N_GY).reshape(IMAGES, SEQ, D)
    feedforward_out = rounded_sum(hidden, down_weight, FF // N_GY, N_GY).reshape(IMAGES, SEQ, D)
    branches = attention_keep.astype(jnp.float32) * attention_out + feedforward_keep.astype(jnp.float32) * feedforward_out
    return (tokens.astype(jnp.float32) + branches * keep_scale).astype(jnp.bfloat16)
```

```python
import jax
import jax.numpy as jnp
from jax import lax
from jax.experimental import pallas as pl
from jax.experimental.pallas import tpu as pltpu
from jax.sharding import Mesh
from jax.sharding import PartitionSpec as P

MESH = pl.DeviceIdType.MESH
AXES = ("yh", "core", "x", "yl", "z")
EPS = 1e-06
KEEP_SCALE = 1.0 / 0.9
BF = jnp.bfloat16
F32 = jnp.float32
N_COPIES = 200
N_LOCAL = 24


def norm_rows(values, gain):
    center = values - jnp.mean(values, axis=-1, keepdims=True)
    variance = jnp.mean(center * center, axis=-1, keepdims=True)
    return center * lax.rsqrt(variance + EPS) * gain


def gelu(v):
    return 0.5 * v * (1.0 + lax.erf(v * 0.7071067811865476))


def kernel(
    tok_ref, gain_ref, qkv_ref, up_ref, qg_ref, kg_ref, wo_ref, wd_ref, ak_ref, fk_ref,
    out_ref,
    ak, fk, w1, w2a, w2b,
    r0, xg, st, xn,
    sq, sm, rq, rm, kq, km, s2q, s2m, r2q, r2m,
    seg, pp, fara, neara, mida, farb, nearb, midb, far2, near2, fin, msg, rout,
    ssem, rsem, lsem,
):
    yh, c, x, yl, z = (lax.axis_index(a) for a in AXES)
    gx = yh * 2 + c
    zh, zl = z // 2, lax.rem(z, 2)

    def ring(v, off):
        return lax.rem(v + off + 4, 4)

    def flip(v, d):
        return lax.rem(v + d, 2)

    xs = [ring(x, o) for o in (0, -1, 1, 2)]
    zs = [ring(z, o) for o in (0, -1, 1, 2)]
    xp, xm, zp, zm = {"x": xs[2]}, {"x": xs[1]}, {"z": zs[2]}, {"z": zs[1]}
    peers = {
        (0, 1): {"core": 1 - c},
        (1, 0): {"yh": 1 - yh},
        (1, 1): {"yh": 1 - yh, "core": 1 - c},
    }
    same = gx == x

    def partner(dy, dz):
        return {
            "yh": x // 2,
            "core": lax.rem(x, 2),
            "x": gx,
            "yl": flip(yl, dy),
            "z": zh * 2 + flip(zl, dz),
        }

    count = [0]
    started = []

    def send(src, dst, dev, start=True):
        i = count[0]
        count[0] += 1
        copy = pltpu.make_async_remote_copy(
            src_ref=src, dst_ref=dst, send_sem=ssem.at[i], recv_sem=rsem.at[i],
            device_id=dev, device_id_type=MESH,
        )
        if start:
            copy.start()
            started.append(copy)
        return copy

    locals_ = [0]

    def load(src, dst):
        i = locals_[0]
        locals_[0] += 1
        copy = pltpu.make_async_copy(src, dst, lsem.at[i])
        copy.start()
        return copy

    loads1, loads2 = [], []
    for t in range(4):
        a, b = t // 2, t % 2
        nat = (b * 2 + a) * 384
        loads1.append(load(qkv_ref.at[pl.ds(nat, 384)], w1.at[a, pl.ds(b * 384, 384), pl.ds(0, 384)]))
        loads1.append(load(up_ref.at[pl.ds(nat, 384)], w1.at[a, pl.ds(b * 384, 384), pl.ds(384, 768)]))
    for t in range(4):
        a, b = t // 2, t % 2
        nat = (b * 2 + a) * 384
        loads2.append(load(wo_ref.at[:, pl.ds(nat, 384)], w2a.at[:, pl.ds(t * 384, 384)]))
        loads2.append(load(wd_ref.at[:, pl.ds(nat, 384)], w2b.at[:, pl.ds(t * 384, 384)]))
    loads3 = [load(ak_ref, ak), load(fk_ref, fk)]

    barrier = pltpu.get_barrier_semaphore()

    def greet(dev):
        pl.semaphore_signal(barrier, inc=1, device_id=dev, device_id_type=MESH)

    for dev in (xp, xm, zp, zm, *peers.values()):
        greet(dev)
    for dy, dz in ((0, 0), (0, 1), (1, 0), (1, 1)):
        greet(partner(dy, dz))
    pl.semaphore_wait(barrier, 11)

    first = {}
    for dy, dz in ((0, 0), (0, 1), (1, 0), (1, 1)):
        whole = dy + dz == 0
        copy = send(tok_ref.at[flip(zl, dz)], r0.at[yl, zl], partner(dy, dz), start=not whole)
        first[dy, dz] = copy
        if whole:
            mine = pltpu.make_async_copy(tok_ref.at[zl], r0.at[yl, zl], lsem.at[N_LOCAL - 1])

            @pl.when(same)
            def _():
                mine.start()
                mine.wait()

            @pl.when(jnp.logical_not(same))
            def _():
                copy.start()

    @pl.when(jnp.logical_not(same))
    def _():
        first[0, 0].wait()

    for key in ((0, 1), (1, 0), (1, 1)):
        first[key].wait_recv()

    xg[x, zh, zl] = jnp.concatenate([r0[0, 0], r0[0, 1], r0[1, 0], r0[1, 1]], axis=1)

    def at(img, zz, lo, n):
        return xg.at[img, zz // 2, lax.rem(zz, 2), pl.ds(lo, n)]

    def both(img, zz, lo, n, devp, devm):
        return (send(at(img, zz, lo, n), at(img, zz, lo, n), devp), send(at(img, zz, lo, n), at(img, zz, lo, n), devm))

    a1 = both(x, z, 0, 64, xp, xm)
    b1 = both(x, z, 64, 64, zp, zm)
    a_out = {0: both(x, z, 0, 64, zp, zm)}
    b_out = {0: both(x, z, 64, 64, xp, xm)}
    a1[0].wait_recv()
    a2p = send(at(xs[1], z, 0, 32), at(xs[1], z, 0, 32), xp)
    b1[0].wait_recv()
    b2p = send(at(x, zs[1], 64, 32), at(x, zs[1], 64, 32), zp)
    a1[1].wait_recv()
    a2m = send(at(xs[2], z, 32, 32), at(xs[2], z, 32, 32), xm)
    b1[1].wait_recv()
    b2m = send(at(x, zs[2], 96, 32), at(x, zs[2], 96, 32), zm)
    a_out[1] = both(xs[1], z, 0, 64, zp, zm)
    b_out[1] = both(x, zs[1], 64, 64, xp, xm)
    a_out[2] = both(xs[2], z, 0, 64, zp, zm)
    b_out[2] = both(x, zs[2], 64, 64, xp, xm)
    a2p.wait_recv()
    a2m.wait_recv()
    a_out[3] = both(xs[3], z, 0, 64, zp, zm)
    b2p.wait_recv()
    b2m.wait_recv()
    b_out[3] = both(x, zs[3], 64, 64, xp, xm)
    last = []
    for k in range(4):
        a_out[k][0].wait_recv()
        last.append(send(at(xs[k], zs[1], 0, 32), at(xs[k], zs[1], 0, 32), zp))
        b_out[k][0].wait_recv()
        last.append(send(at(xs[1], zs[k], 64, 32), at(xs[1], zs[k], 64, 32), xp))
        a_out[k][1].wait_recv()
        last.append(send(at(xs[k], zs[2], 32, 32), at(xs[k], zs[2], 32, 32), zm))
        b_out[k][1].wait_recv()
        last.append(send(at(xs[2], zs[k], 96, 32), at(xs[2], zs[k], 96, 32), xm))
    for copy in last:
        copy.wait_recv()

    eye = lax.broadcasted_iota(jnp.int32, (128, 128), 0) == lax.broadcasted_iota(jnp.int32, (128, 128), 1)

    def to_row(col):
        return jnp.sum(jnp.where(eye, jnp.broadcast_to(col, (128, 128)), 0.0), axis=0, keepdims=True)

    def to_col(row):
        return jnp.sum(jnp.where(eye, jnp.broadcast_to(row, (128, 128)), 0.0), axis=1, keepdims=True)

    @pl.loop(0, 4)
    def _(m):
        for h in range(2):
            lo = xg[m, 0, h].astype(F32)
            hi = xg[m, 1, h].astype(F32)
            mean = (jnp.sum(lo, axis=1, keepdims=True) + jnp.sum(hi, axis=1, keepdims=True)) * (1.0 / 1536.0)
            dl, dh = lo - mean, hi - mean
            spread = jnp.sum(dl * dl, axis=1, keepdims=True) + jnp.sum(dh * dh, axis=1, keepdims=True)
            st[0, m, h, 0:1] = to_row(mean)
            st[0, m, h, 1:2] = to_row(spread)

    shared = [send(st.at[0], st.at[d[0] * 2 + d[1]], peers[d]) for d in peers]
    for copy in shared:
        copy.wait_recv()
    for copy in loads1:
        copy.wait()

    def first_matmul(m, put):
        for h in range(2):
            means = [st[k, m, h, 0:1] for k in range(4)]
            mean = (means[0] + means[1] + means[2] + means[3]) * 0.25
            spread = sum(st[k, m, h, 1:2] + 1536.0 * (means[k] - mean) * (means[k] - mean) for k in range(4))
            scale = lax.rsqrt(spread * (1.0 / 6144.0) + EPS)
            mean_c, scale_c = to_col(mean), to_col(scale)
            for a in range(2):
                for b in range(2):
                    g = gain_ref[gx, 0:1, (b * 2 + a) * 384 : (b * 2 + a + 1) * 384]
                    v = xg[m, a, h, :, b * 384 : (b + 1) * 384].astype(F32)
                    xn[a, h * 128 : (h + 1) * 128, b * 384 : (b + 1) * 384] = ((v - mean_c) * scale_c * g).astype(BF)
        for n in range(3):
            cols = slice(n * 384, (n + 1) * 384)
            y = jnp.dot(xn[0], w1[0, :, cols], preferred_element_type=F32)
            y = y + jnp.dot(xn[1], w1[1, :, cols], preferred_element_type=F32)
            put(n, y)

    def put_into(q, mlp, lead, kind):
        def put(n, y):
            if n == 0:
                q[lead] = y.astype(kind)
            else:
                for h in range(2):
                    for r in range(4):
                        rows = y[h * 128 + r * 32 : h * 128 + (r + 1) * 32].astype(kind)
                        mlp[lead, r, h * 32 : (h + 1) * 32, (n - 1) * 384 : n * 384] = rows
        return put

    far_img = lambda dyh, dc: flip(yh, dyh) * 2 + flip(c, dc)
    pair = []
    for dyh in (1, 0):
        first_matmul(far_img(dyh, 1), put_into(sq, sm, dyh, BF))
        d2d = (send(sq.at[dyh], rq.at[dyh], peers[0, 1]), send(sm.at[dyh], rm.at[dyh], peers[0, 1]))
        pair.append(d2d)
        first_matmul(far_img(dyh, 0), put_into(kq, km, dyh, F32))
        if dyh == 1:
            d2d[0].wait_recv()
            s2q[...] = (kq[1] + rq[1].astype(F32)).astype(BF)
            across_q = send(s2q, r2q, peers[1, 0])
            d2d[1].wait_recv()
            across_m = []
            for r in range(4):
                s2m[r] = (km[1, r] + rm[1, r].astype(F32)).astype(BF)
                across_m.append(send(s2m.at[r], r2m.at[r], peers[1, 0]))

    pair[1][0].wait_recv()
    pair[1][1].wait_recv()
    across_q.wait_recv()
    mine_q = kq[0] + rq[0].astype(F32) + r2q[...].astype(F32)
    queries = norm_rows(mine_q[:, 0:128], qg_ref[...]).astype(BF)
    keys = norm_rows(mine_q[:, 128:256], kg_ref[...]).astype(BF)
    values = mine_q[:, 256:384].astype(BF)
    scores = lax.dot_general(queries, keys, (((1,), (1,)), ((), ())), preferred_element_type=F32) * (128 ** -0.5)
    raised = jnp.exp(scores)
    weights = (raised / jnp.sum(raised, axis=-1, keepdims=True)).astype(BF)
    attended = jnp.dot(weights, values, preferred_element_type=F32).astype(BF)
    for h in range(2):
        for r in range(4):
            seg[r, gx, h, :, 0:128] = attended[h * 128 + r * 32 : h * 128 + (r + 1) * 32]

    order = (0, 2, 1, 3)
    spread_y, spread_c = {}, {}
    for r in order:
        across_m[r].wait_recv()
        v = gelu(km[0, r] + rm[0, r].astype(F32) + r2m[r].astype(F32)).astype(BF)
        for h in range(2):
            seg[r, gx, h, :, 128:896] = v[h * 32 : (h + 1) * 32]
        spread_y[r] = send(seg.at[r, gx], seg.at[r, gx], peers[1, 0])
        spread_c[r] = send(seg.at[r, gx], seg.at[r, gx], peers[0, 1])

    for copy in loads2:
        copy.wait()

    def ring_rs(part, devp, devm, dest, far, near, out):
        f0 = send(part(0, dest[3]), far.at[0], devp)
        f1 = send(part(1, dest[3]), far.at[1], devm)
        o1 = send(part(1, dest[2]), near.at[0, 1], devp)
        o0 = send(part(0, dest[1]), near.at[1, 0], devm)
        late = []

        def middle():
            f0.wait_recv()
            ref = part(0, dest[2])
            ref[...] = (ref[...].astype(F32) + far[0].astype(F32)).astype(BF)
            late.append(send(ref, near.at[0, 0], devp))
            f1.wait_recv()
            ref = part(1, dest[1])
            ref[...] = (ref[...].astype(F32) + far[1].astype(F32)).astype(BF)
            late.append(send(ref, near.at[1, 1], devm))

        def end():
            for copy in (o1, o0, *late):
                copy.wait_recv()
            for br in range(2):
                total = part(br, dest[0])[...].astype(F32) + near[0, br].astype(F32) + near[1, br].astype(F32)
                out[br] = total.astype(BF)

        return middle, end

    def chunk_matmul(r):
        spread_c[r].wait_recv()
        forwards[r].wait_recv()
        left = seg[r].reshape(256, 896)
        for a in range(2):
            cols = slice(a * 768, (a + 1) * 768)
            y = jnp.dot(left[:, 0:128], w2a[:, cols], preferred_element_type=F32)
            pp[r, 0, a] = y.astype(BF).reshape(4, 2, 32, 768)
            y = jnp.dot(left[:, 128:896], w2b[:, cols], preferred_element_type=F32)
            pp[r, 1, a] = y.astype(BF).reshape(4, 2, 32, 768)

    def stage1(r):
        if r < 2:
            part = lambda br, d: pp.at[r, br, d // 2, :, lax.rem(d, 2)]
            return ring_rs(part, zp, zm, zs, fara.at[r], neara.at[r], mida.at[r])
        part = lambda br, d: pp.at[r, br, :, d]
        return ring_rs(part, xp, xm, xs, farb.at[r - 2], nearb.at[r - 2], midb.at[r - 2])

    def stage2(r):
        if r < 2:
            part = lambda br, d: mida.at[r, br, d]
            return ring_rs(part, xp, xm, xs, far2.at[r], near2.at[r], fin.at[r])
        part = lambda br, d: midb.at[r - 2, br, d // 2, lax.rem(d, 2)]
        return ring_rs(part, zp, zm, zs, far2.at[r], near2.at[r], fin.at[r])

    home = {}

    def deliver(r):
        for q in range(4):
            cols = slice(q * 192, (q + 1) * 192)
            msg[r, q] = jnp.concatenate([fin[r, 0, :, cols], fin[r, 1, :, cols]], axis=1)
        for dy, dz in ((0, 0), (0, 1), (1, 0), (1, 1)):
            whole = dy + dz == 0
            q = flip(yl, dy) * 2 + flip(zl, dz)
            copy = send(msg.at[r, q], rout.at[yl, zl, r], partner(dy, dz), start=not whole)
            home[r, dy, dz] = copy
            if whole:
                @pl.when(same)
                def _():
                    rout[yl, zl, r] = msg[r, q]

                @pl.when(jnp.logical_not(same))
                def _():
                    copy.start()

    forwards = {}
    mids, ends, mids2, ends2 = {}, {}, {}, {}

    def begin(r):
        mids[r], ends[r] = stage1(r)

    def turn(r):
        ends[r]()
        mids2[r], ends2[r] = stage2(r)

    def close(r):
        ends2[r]()
        deliver(r)

    for r in order:
        spread_y[r].wait_recv()
        forwards[r] = send(seg.at[r, far_img(1, 0)], seg.at[r, far_img(1, 0)], peers[0, 1])
        if r == 0 or r == 2:
            chunk_matmul(r)
            begin(r)
    mids[0]()
    mids[2]()
    chunk_matmul(1)
    begin(1)
    chunk_matmul(3)
    begin(3)
    turn(0)
    turn(2)
    mids[1]()
    mids[3]()
    mids2[0]()
    mids2[2]()
    close(0)
    close(2)
    turn(1)
    turn(3)
    mids2[1]()
    mids2[3]()
    close(1)
    close(3)

    for copy in loads3:
        copy.wait()
    for r in order:
        for dy, dz in ((0, 1), (1, 0), (1, 1)):
            home[r, dy, dz].wait_recv()

        @pl.when(jnp.logical_not(same))
        def _():
            home[r, 0, 0].wait()

        for h in range(2):
            total = rout[0, h, r].astype(F32) + rout[1, h, r].astype(F32)
            rows = slice(r * 32, (r + 1) * 32)
            branches = ak[h, rows].astype(F32) * total[:, 0:192] + fk[h, rows].astype(F32) * total[:, 192:384]
            out_ref[h, rows] = (tok_ref[h, rows].astype(F32) + branches * KEEP_SCALE).astype(BF)

    for copy in started:
        copy.wait_send()


def per_device(tokens, norm_gain, qkv_weight, up_weight, query_gain, key_gain, out_weight, down_weight, ak, fk):
    vm = pl.BlockSpec(memory_space=pltpu.VMEM)
    hbm = pl.BlockSpec(memory_space=pl.ANY)
    V = pltpu.VMEM
    scratch = [
        V((2, 128, 192), jnp.int32), V((2, 128, 192), jnp.int32),
        V((2, 768, 1152), BF), V((128, 1536), BF), V((768, 1536), BF),
        V((2, 2, 128, 192), BF), V((4, 2, 2, 128, 768), BF), V((4, 4, 2, 8, 128), F32), V((2, 256, 768), BF),
        V((2, 256, 384), BF), V((2, 4, 64, 768), BF), V((2, 256, 384), BF), V((2, 4, 64, 768), BF),
        V((2, 256, 384), F32), V((2, 4, 64, 768), F32),
        V((256, 384), BF), V((4, 64, 768), BF), V((256, 384), BF), V((4, 64, 768), BF),
        V((4, 4, 2, 32, 896), BF), V((4, 2, 2, 4, 2, 32, 768), BF),
        V((2, 2, 4, 32, 768), BF), V((2, 2, 2, 4, 32, 768), BF), V((2, 2, 4, 32, 768), BF),
        V((2, 2, 2, 2, 32, 768), BF), V((2, 2, 2, 2, 2, 32, 768), BF), V((2, 2, 2, 2, 32, 768), BF),
        V((4, 2, 32, 768), BF), V((4, 2, 2, 32, 768), BF), V((4, 2, 32, 768), BF),
        V((4, 4, 32, 384), BF), V((2, 2, 4, 32, 384), BF),
        pltpu.SemaphoreType.DMA((N_COPIES,)), pltpu.SemaphoreType.DMA((N_COPIES,)), pltpu.SemaphoreType.DMA((N_LOCAL,)),
    ]
    out = pl.pallas_call(
        kernel,
        out_shape=jax.ShapeDtypeStruct((2, 128, 192), BF),
        in_specs=[vm, vm, hbm, hbm, vm, vm, hbm, hbm, hbm, hbm],
        out_specs=vm,
        scratch_shapes=scratch,
        compiler_params=pltpu.CompilerParams(collective_id=0, has_side_effects=True, vmem_limit_bytes=60000 * 1024),
        name="block",
    )(
        tokens.reshape(2, 128, 192),
        norm_gain.reshape(4, 1, 1536),
        qkv_weight.reshape(1536, 384),
        up_weight,
        query_gain.reshape(1, 128),
        key_gain.reshape(1, 128),
        out_weight,
        down_weight,
        ak.reshape(2, 128, 192),
        fk.reshape(2, 128, 192),
    )
    return out.reshape(1, 256, 192)


def solution(mesh):
    split = Mesh(mesh.devices.reshape(2, 2, 4, 2, 4), AXES)
    gx, gy = ("yh", "core"), ("x", "yl", "z")
    placed = (
        P(gx, None, gy), P(), P(gx, None, gy), P(gx, gy), P(), P(), P(gy, gx), P(gy, gx), P(gx, None, gy), P(gx, None, gy),
    )
    return jax.shard_map(per_device, mesh=split, in_specs=placed, out_specs=P(gx, None, gy), check_vma=False)
```

```python
import jax
import jax.numpy as jnp
from jax import lax
from jax.experimental import pallas as pl
from jax.experimental.pallas import tpu as pltpu
from jax.sharding import Mesh
from jax.sharding import PartitionSpec as P

MESH = pl.DeviceIdType.MESH
AXES = ("yh", "core", "x", "yl", "z")
EPS = 1e-06
KEEP_SCALE = 1.0 / 0.9
BF = jnp.bfloat16
F32 = jnp.float32
N_COPIES = 200
N_LOCAL = 32
Z_FIRST = (0,)


def norm_rows(values, gain):
    center = values - jnp.mean(values, axis=-1, keepdims=True)
    variance = jnp.mean(center * center, axis=-1, keepdims=True)
    return center * lax.rsqrt(variance + EPS) * gain


def gelu(v):
    return 0.5 * v * (1.0 + lax.erf(v * 0.7071067811865476))


def kernel(
    tok_ref, gain_ref, qkv_ref, up_ref, qg_ref, kg_ref, wo_ref, wd_ref, ak_ref, fk_ref,
    out_ref,
    ak, fk, w1, w2a, w2b,
    r0, xg, st, xn,
    sq, sm, rq, rm, kq, km, s2q, s2m, r2q, r2m,
    seg, asend, att, pa, far0, near0, fin0, pp,
    fara, neara, mida, farb, nearb, midb, far2, near2, fin, msg, rout, asem_s, asem_r,
    ssem, rsem, lsem,
):
    yh, c, x, yl, z = (lax.axis_index(a) for a in AXES)
    gx = yh * 2 + c
    zh, zl = z // 2, lax.rem(z, 2)

    def ring(v, off):
        return lax.rem(v + off + 4, 4)

    def flip(v, d):
        return lax.rem(v + d, 2)

    xs = [ring(x, o) for o in (0, -1, 1, 2)]
    zs = [ring(z, o) for o in (0, -1, 1, 2)]
    xp, xm, zp, zm = {"x": xs[2]}, {"x": xs[1]}, {"z": zs[2]}, {"z": zs[1]}
    peers = {
        (0, 1): {"core": 1 - c},
        (1, 0): {"yh": 1 - yh},
        (1, 1): {"yh": 1 - yh, "core": 1 - c},
    }
    same = gx == x

    def partner(dy, dz):
        return {
            "yh": x // 2,
            "core": lax.rem(x, 2),
            "x": gx,
            "yl": flip(yl, dy),
            "z": zh * 2 + flip(zl, dz),
        }

    count = [0]
    started = []

    def send(src, dst, dev, start=True):
        i = count[0]
        count[0] += 1
        copy = pltpu.make_async_remote_copy(
            src_ref=src, dst_ref=dst, send_sem=ssem.at[i], recv_sem=rsem.at[i],
            device_id=dev, device_id_type=MESH,
        )
        if start:
            copy.start()
            started.append(copy)
        return copy

    locals_ = [0]

    def load(src, dst):
        i = locals_[0]
        locals_[0] += 1
        copy = pltpu.make_async_copy(src, dst, lsem.at[i])
        copy.start()
        return copy

    loads1, loads2, loads4 = [], [], []
    for t in range(4):
        a, b = t // 2, t % 2
        nat = (b * 2 + a) * 384
        for k in range(3):
            loads1.append(load(qkv_ref.at[k, pl.ds(nat, 384)], w1.at[a, pl.ds(b * 384, 384), pl.ds(k * 128, 128)]))
        loads1.append(load(up_ref.at[pl.ds(nat, 384)], w1.at[a, pl.ds(b * 384, 384), pl.ds(384, 768)]))
    for t in range(4):
        a, b = t // 2, t % 2
        nat = (b * 2 + a) * 384
        loads4.append(load(wo_ref.at[:, pl.ds(nat, 384)], w2a.at[x, :, pl.ds(t * 384, 384)]))
        loads2.append(load(wd_ref.at[:, pl.ds(nat, 384)], w2b.at[:, pl.ds(t * 384, 384)]))
    loads3 = [load(ak_ref, ak), load(fk_ref, fk)]

    barrier = pltpu.get_barrier_semaphore()

    def greet(dev):
        pl.semaphore_signal(barrier, inc=1, device_id=dev, device_id_type=MESH)

    for dev in (xp, xm, zp, zm, *peers.values()):
        greet(dev)
    for dy, dz in ((0, 0), (0, 1), (1, 0), (1, 1)):
        greet(partner(dy, dz))
    for k in range(4):
        greet({"yh": x // 2, "core": lax.rem(x, 2), "x": k})
    pl.semaphore_wait(barrier, 15)

    def lanes(h):
        return pl.ds(pl.multiple_of(h * 128, 128), 128)

    first = {}
    for dy, dz in ((0, 0), (0, 1), (1, 0), (1, 1)):
        whole = dy + dz == 0
        copy = send(tok_ref.at[:, lanes(flip(zl, dz))], r0.at[yl, zl], partner(dy, dz), start=not whole)
        first[dy, dz] = copy
        if whole:
            mine = pltpu.make_async_copy(tok_ref.at[:, lanes(zl)], r0.at[yl, zl], lsem.at[N_LOCAL - 1])

            @pl.when(same)
            def _():
                mine.start()
                mine.wait()

            @pl.when(jnp.logical_not(same))
            def _():
                copy.start()

    @pl.when(jnp.logical_not(same))
    def _():
        first[0, 0].wait()

    for key in ((0, 1), (1, 0), (1, 1)):
        first[key].wait_recv()

    xg[x, zh, zl] = r0[...].reshape(768, 128).T

    def at(img, zz, lo, n):
        return xg.at[img, zz // 2, lax.rem(zz, 2), pl.ds(lo, n)]

    def both(img, zz, lo, n, devp, devm):
        return (send(at(img, zz, lo, n), at(img, zz, lo, n), devp), send(at(img, zz, lo, n), at(img, zz, lo, n), devm))

    a1 = both(x, z, 0, 64, xp, xm)
    b1 = both(x, z, 64, 64, zp, zm)
    a_out = {0: both(x, z, 0, 64, zp, zm)}
    b_out = {0: both(x, z, 64, 64, xp, xm)}
    a1[0].wait_recv()
    a2p = send(at(xs[1], z, 0, 32), at(xs[1], z, 0, 32), xp)
    b1[0].wait_recv()
    b2p = send(at(x, zs[1], 64, 32), at(x, zs[1], 64, 32), zp)
    a1[1].wait_recv()
    a2m = send(at(xs[2], z, 32, 32), at(xs[2], z, 32, 32), xm)
    b1[1].wait_recv()
    b2m = send(at(x, zs[2], 96, 32), at(x, zs[2], 96, 32), zm)
    a_out[1] = both(xs[1], z, 0, 64, zp, zm)
    b_out[1] = both(x, zs[1], 64, 64, xp, xm)
    a_out[2] = both(xs[2], z, 0, 64, zp, zm)
    b_out[2] = both(x, zs[2], 64, 64, xp, xm)
    a2p.wait_recv()
    a2m.wait_recv()
    a_out[3] = both(xs[3], z, 0, 64, zp, zm)
    b2p.wait_recv()
    b2m.wait_recv()
    b_out[3] = both(x, zs[3], 64, 64, xp, xm)
    last = []
    for k in range(4):
        a_out[k][0].wait_recv()
        last.append(send(at(xs[k], zs[1], 0, 32), at(xs[k], zs[1], 0, 32), zp))
        b_out[k][0].wait_recv()
        last.append(send(at(xs[1], zs[k], 64, 32), at(xs[1], zs[k], 64, 32), xp))
        a_out[k][1].wait_recv()
        last.append(send(at(xs[k], zs[2], 32, 32), at(xs[k], zs[2], 32, 32), zm))
        b_out[k][1].wait_recv()
        last.append(send(at(xs[2], zs[k], 96, 32), at(xs[2], zs[k], 96, 32), xm))
    for copy in last:
        copy.wait_recv()

    eye = lax.broadcasted_iota(jnp.int32, (128, 128), 0) == lax.broadcasted_iota(jnp.int32, (128, 128), 1)

    def to_row(col):
        return jnp.sum(jnp.where(eye, jnp.broadcast_to(col, (128, 128)), 0.0), axis=0, keepdims=True)

    def to_col(row):
        return jnp.sum(jnp.where(eye, jnp.broadcast_to(row, (128, 128)), 0.0), axis=1, keepdims=True)

    @pl.loop(0, 4)
    def _(m):
        for h in range(2):
            lo = xg[m, 0, h].astype(F32)
            hi = xg[m, 1, h].astype(F32)
            mean = (jnp.sum(lo, axis=1, keepdims=True) + jnp.sum(hi, axis=1, keepdims=True)) * (1.0 / 1536.0)
            dl, dh = lo - mean, hi - mean
            spread = jnp.sum(dl * dl, axis=1, keepdims=True) + jnp.sum(dh * dh, axis=1, keepdims=True)
            st[0, m, h, 0:1] = to_row(mean)
            st[0, m, h, 1:2] = to_row(spread)

    for copy in loads4:
        copy.wait()
    wo1 = (send(w2a.at[x], w2a.at[x], xp), send(w2a.at[x], w2a.at[x], xm))
    shared = [send(st.at[0], st.at[d[0] * 2 + d[1]], peers[d]) for d in peers]
    for copy in shared:
        copy.wait_recv()
    for copy in loads1:
        copy.wait()

    def first_matmul(m, put):
        for h in range(2):
            means = [st[k, m, h, 0:1] for k in range(4)]
            mean = (means[0] + means[1] + means[2] + means[3]) * 0.25
            spread = sum(st[k, m, h, 1:2] + 1536.0 * (means[k] - mean) * (means[k] - mean) for k in range(4))
            scale = lax.rsqrt(spread * (1.0 / 6144.0) + EPS)
            mean_c, scale_c = to_col(mean), to_col(scale)
            for a in range(2):
                for b in range(2):
                    g = gain_ref[gx, 0:1, (b * 2 + a) * 384 : (b * 2 + a + 1) * 384]
                    v = xg[m, a, h, :, b * 384 : (b + 1) * 384].astype(F32)
                    xn[a, h * 128 : (h + 1) * 128, b * 384 : (b + 1) * 384] = ((v - mean_c) * scale_c * g).astype(BF)
        for n in range(3):
            cols = slice(n * 384, (n + 1) * 384)
            y = jnp.dot(xn[0], w1[0, :, cols], preferred_element_type=F32)
            y = y + jnp.dot(xn[1], w1[1, :, cols], preferred_element_type=F32)
            put(n, y)

    def put_into(q, mlp, lead, kind):
        def put(n, y):
            if n == 0:
                q[lead] = y.astype(kind)
            else:
                for h in range(2):
                    for r in range(4):
                        rows = y[h * 128 + r * 32 : h * 128 + (r + 1) * 32].astype(kind)
                        mlp[lead, r, h * 32 : (h + 1) * 32, (n - 1) * 384 : n * 384] = rows
        return put

    far_img = lambda dyh, dc: flip(yh, dyh) * 2 + flip(c, dc)
    pair = []
    for dyh in (1, 0):
        first_matmul(far_img(dyh, 1), put_into(sq, sm, dyh, BF))
        d2d = (send(sq.at[dyh], rq.at[dyh], peers[0, 1]), send(sm.at[dyh], rm.at[dyh], peers[0, 1]))
        pair.append(d2d)
        first_matmul(far_img(dyh, 0), put_into(kq, km, dyh, F32))
        if dyh == 1:
            d2d[0].wait_recv()
            s2q[...] = (kq[1] + rq[1].astype(F32)).astype(BF)
            across_q = send(s2q, r2q, peers[1, 0])
            d2d[1].wait_recv()
            across_m = []
            for r in range(4):
                s2m[r] = (km[1, r] + rm[1, r].astype(F32)).astype(BF)
                across_m.append(send(s2m.at[r], r2m.at[r], peers[1, 0]))

    wo1[0].wait_recv()
    wo2p = send(w2a.at[xs[1], pl.ds(0, 64)], w2a.at[xs[1], pl.ds(0, 64)], xp)
    wo1[1].wait_recv()
    wo2m = send(w2a.at[xs[2], pl.ds(64, 64)], w2a.at[xs[2], pl.ds(64, 64)], xm)
    pair[1][0].wait_recv()
    pair[1][1].wait_recv()
    across_q.wait_recv()
    mine_q = kq[0] + rq[0].astype(F32) + r2q[...].astype(F32)
    queries = norm_rows(mine_q[:, 0:128], qg_ref[...]).astype(BF)
    keys = norm_rows(mine_q[:, 128:256], kg_ref[...]).astype(BF)
    values = mine_q[:, 256:384].astype(BF)
    scores = lax.dot_general(queries, keys, (((1,), (1,)), ((), ())), preferred_element_type=F32) * (128 ** -0.5)
    raised = jnp.exp(scores)
    weights = (raised / jnp.sum(raised, axis=-1, keepdims=True)).astype(BF)
    attended = jnp.dot(weights, values, preferred_element_type=F32).astype(BF)
    asend[...] = attended

    def to_row_owner(dyh, dc):
        i = dyh * 2 + dc
        dev = {"yh": flip(yh, dyh), "core": flip(c, dc), "x": gx}
        return pltpu.make_async_remote_copy(
            src_ref=asend, dst_ref=att.at[x], send_sem=asem_s.at[i], recv_sem=asem_r.at[x],
            device_id=dev, device_id_type=MESH,
        )

    @pl.when(same)
    def _():
        pltpu.make_async_copy(asend, att.at[x], asem_r.at[x]).start()

    @pl.when(jnp.logical_not(same))
    def _():
        to_row_owner(0, 0).start()

    for d in peers:
        to_row_owner(*d).start()

    order = (0, 2, 1, 3)
    spread_y, spread_c = {}, {}
    for r in order:
        across_m[r].wait_recv()
        v = gelu(km[0, r] + rm[0, r].astype(F32) + r2m[r].astype(F32)).astype(BF)
        for h in range(2):
            seg[r, gx, h] = v[h * 32 : (h + 1) * 32]
        spread_y[r] = send(seg.at[r, gx], seg.at[r, gx], peers[1, 0])
        spread_c[r] = send(seg.at[r, gx], seg.at[r, gx], peers[0, 1])

    for copy in loads2:
        copy.wait()

    def ring_rs(part, devp, devm, dest, far, near, out):
        f0 = send(part(0, dest[3]), far.at[0], devp)
        f1 = send(part(1, dest[3]), far.at[1], devm)
        o1 = send(part(1, dest[2]), near.at[0, 1], devp)
        o0 = send(part(0, dest[1]), near.at[1, 0], devm)
        late = []

        def middle():
            f0.wait_recv()
            ref = part(0, dest[2])
            ref[...] = (ref[...].astype(F32) + far[0].astype(F32)).astype(BF)
            late.append(send(ref, near.at[0, 0], devp))
            f1.wait_recv()
            ref = part(1, dest[1])
            ref[...] = (ref[...].astype(F32) + far[1].astype(F32)).astype(BF)
            late.append(send(ref, near.at[1, 1], devm))

        def end():
            for copy in (o1, o0, *late):
                copy.wait_recv()
            for br in range(2):
                total = part(br, dest[0])[...].astype(F32) + near[0, br].astype(F32) + near[1, br].astype(F32)
                out[br] = total.astype(BF)

        return middle, end

    def attended_matmul():
        for k in range(4):
            pltpu.make_async_remote_copy(
                src_ref=asend, dst_ref=att.at[k], send_sem=asem_s.at[0], recv_sem=asem_r.at[k],
                device_id=peers[0, 1], device_id_type=MESH,
            ).wait_recv()
        wo2p.wait_recv()
        wo2m.wait_recv()
        left = jnp.concatenate([att[k] for k in range(4)], axis=1)
        for a in range(2):
            right = w2a[:, :, a * 768 : (a + 1) * 768].reshape(512, 768)
            y = jnp.dot(left, right, preferred_element_type=F32)
            pa[a] = y.astype(BF).reshape(2, 128, 768)

    def chunk_matmul(r):
        spread_c[r].wait_recv()
        forwards[r].wait_recv()
        left = seg[r].reshape(256, 768)
        for a in range(2):
            y = jnp.dot(left, w2b[:, a * 768 : (a + 1) * 768], preferred_element_type=F32)
            pp[r, a] = y.astype(BF).reshape(4, 2, 32, 768)

    def stage0():
        part = lambda k, d: pa.at[d // 2, lax.rem(d, 2), pl.ds(k * 64, 64)]
        return ring_rs(part, zp, zm, zs, far0, near0, fin0)

    def stage1(r):
        i = index[r]
        if r in Z_FIRST:
            part = lambda k, d: pp.at[r, d // 2, pl.ds(k * 2, 2), lax.rem(d, 2)]
            return ring_rs(part, zp, zm, zs, fara.at[i], neara.at[i], mida.at[i])
        part = lambda k, d: pp.at[r, k, d]
        return ring_rs(part, xp, xm, xs, farb.at[i], nearb.at[i], midb.at[i])

    def stage2(r):
        i = index[r]
        if r in Z_FIRST:
            part = lambda k, d: mida.at[i, d // 2, lax.rem(d, 2), pl.ds(k * 16, 16)]
            return ring_rs(part, xp, xm, xs, far2.at[r], near2.at[r], fin.at[r])
        part = lambda k, d: midb.at[i, d // 2, lax.rem(d, 2), pl.ds(k * 16, 16)]
        return ring_rs(part, zp, zm, zs, far2.at[r], near2.at[r], fin.at[r])

    index = {}
    for r in range(4):
        index[r] = sum((q in Z_FIRST) == (r in Z_FIRST) for q in range(r))

    home = {}

    def deliver(r):
        left = fin[r].reshape(32, 768)
        for q in range(4):
            cols = slice(q * 192, (q + 1) * 192)
            msg[r, q] = jnp.concatenate([fin0[r // 2, (r % 2) * 32 : (r % 2) * 32 + 32, cols], left[:, cols]], axis=1)
        for dy, dz in ((0, 0), (0, 1), (1, 0), (1, 1)):
            whole = dy + dz == 0
            q = flip(yl, dy) * 2 + flip(zl, dz)
            copy = send(msg.at[r, q], rout.at[yl, zl, r], partner(dy, dz), start=not whole)
            home[r, dy, dz] = copy
            if whole:
                @pl.when(same)
                def _():
                    rout[yl, zl, r] = msg[r, q]

                @pl.when(jnp.logical_not(same))
                def _():
                    copy.start()

    forwards = {}
    mids, ends, mids2, ends2 = {}, {}, {}, {}

    def begin(r):
        mids[r], ends[r] = stage1(r)

    def turn(r):
        ends[r]()
        mids2[r], ends2[r] = stage2(r)

    def close(r):
        ends2[r]()
        deliver(r)

    attended_matmul()
    mid0, end0 = stage0()
    for r in order:
        spread_y[r].wait_recv()
        forwards[r] = send(seg.at[r, far_img(1, 0)], seg.at[r, far_img(1, 0)], peers[0, 1])
        if r == order[0]:
            chunk_matmul(r)
            begin(r)
            mid0()
        if r == order[1]:
            chunk_matmul(r)
            begin(r)
    mids[order[0]]()
    mids[order[1]]()
    end0()
    chunk_matmul(order[2])
    begin(order[2])
    turn(order[0])
    chunk_matmul(order[3])
    begin(order[3])
    turn(order[1])
    mids[order[2]]()
    mids2[order[0]]()
    mids[order[3]]()
    mids2[order[1]]()
    close(order[0])
    turn(order[2])
    close(order[1])
    turn(order[3])
    mids2[order[2]]()
    mids2[order[3]]()
    close(order[2])
    close(order[3])

    for copy in loads3:
        copy.wait()
    for r in order:
        for dy, dz in ((0, 1), (1, 0), (1, 1)):
            home[r, dy, dz].wait_recv()

        @pl.when(jnp.logical_not(same))
        def _():
            home[r, 0, 0].wait()

    for h in range(2):
        total = (rout[0, h].astype(F32) + rout[1, h].astype(F32)).reshape(128, 384).T
        cols = slice(h * 128, (h + 1) * 128)
        branches = ak[:, cols].astype(F32) * total[0:192] + fk[:, cols].astype(F32) * total[192:384]
        out_ref[:, cols] = (tok_ref[:, cols].astype(F32) + branches * KEEP_SCALE).astype(BF)

    @pl.when(jnp.logical_not(same))
    def _():
        to_row_owner(0, 0).wait_send()

    for d in peers:
        to_row_owner(*d).wait_send()
    for copy in started:
        copy.wait_send()


def per_device(tokens, norm_gain, qkv_weight, up_weight, query_gain, key_gain, out_weight, down_weight, ak, fk):
    vm = pl.BlockSpec(memory_space=pltpu.VMEM)
    hbm = pl.BlockSpec(memory_space=pl.ANY)
    V = pltpu.VMEM
    n = len(Z_FIRST)
    scratch = [
        V((192, 256), jnp.int32), V((192, 256), jnp.int32),
        V((2, 768, 1152), BF), V((4, 128, 1536), BF), V((768, 1536), BF),
        V((2, 2, 192, 128), BF), V((4, 2, 2, 128, 768), BF), V((4, 4, 2, 8, 128), F32), V((2, 256, 768), BF),
        V((2, 256, 384), BF), V((2, 4, 64, 768), BF), V((2, 256, 384), BF), V((2, 4, 64, 768), BF),
        V((2, 256, 384), F32), V((2, 4, 64, 768), F32),
        V((256, 384), BF), V((4, 64, 768), BF), V((256, 384), BF), V((4, 64, 768), BF),
        V((4, 4, 2, 32, 768), BF), V((256, 128), BF), V((4, 256, 128), BF),
        V((2, 2, 128, 768), BF), V((2, 64, 768), BF), V((2, 2, 64, 768), BF), V((2, 64, 768), BF),
        V((4, 2, 4, 2, 32, 768), BF),
        V((n, 2, 2, 32, 768), BF), V((n, 2, 2, 2, 32, 768), BF), V((n, 2, 2, 32, 768), BF),
        V((4 - n, 2, 2, 32, 768), BF), V((4 - n, 2, 2, 2, 32, 768), BF), V((4 - n, 2, 2, 32, 768), BF),
        V((4, 2, 16, 768), BF), V((4, 2, 2, 16, 768), BF), V((4, 2, 16, 768), BF),
        V((4, 4, 32, 384), BF), V((2, 2, 4, 32, 384), BF),
        pltpu.SemaphoreType.DMA((4,)), pltpu.SemaphoreType.DMA((4,)),
        pltpu.SemaphoreType.DMA((N_COPIES,)), pltpu.SemaphoreType.DMA((N_COPIES,)), pltpu.SemaphoreType.DMA((N_LOCAL,)),
    ]
    out = pl.pallas_call(
        kernel,
        out_shape=jax.ShapeDtypeStruct((192, 256), BF),
        in_specs=[vm, vm, hbm, hbm, vm, vm, hbm, hbm, hbm, hbm],
        out_specs=vm,
        scratch_shapes=scratch,
        compiler_params=pltpu.CompilerParams(collective_id=0, has_side_effects=True, vmem_limit_bytes=60000 * 1024),
        name="block",
    )(
        tokens[0].T,
        norm_gain.reshape(4, 1, 1536),
        qkv_weight.transpose(1, 0, 2),
        up_weight,
        query_gain.reshape(1, 128),
        key_gain.reshape(1, 128),
        out_weight,
        down_weight,
        ak[0].T,
        fk[0].T,
    )
    return out.T[None]


def solution(mesh):
    split = Mesh(mesh.devices.reshape(2, 2, 4, 2, 4), AXES)
    gx, gy = ("yh", "core"), ("x", "yl", "z")
    placed = (
        P(gx, None, gy), P(), P(gx, None, gy), P(gx, gy), P(), P(), P(gy, gx), P(gy, gx), P(gx, None, gy), P(gx, None, gy),
    )
    return jax.shard_map(per_device, mesh=split, in_specs=placed, out_specs=P(gx, None, gy), check_vma=False)
```

```python
import jax
import jax.numpy as jnp
from jax import lax
from jax.experimental import pallas as pl
from jax.experimental.pallas import tpu as pltpu
from jax.sharding import Mesh
from jax.sharding import PartitionSpec as P

MESH = pl.DeviceIdType.MESH
AXES = ("yh", "core", "x", "yl", "z")
EPS = 1e-06
KEEP_SCALE = 1.0 / 0.9
BF = jnp.bfloat16
F32 = jnp.float32
N_COPIES = 224
N_LOCAL = 32


def norm_rows(values, gain):
    center = values - jnp.mean(values, axis=-1, keepdims=True)
    variance = jnp.mean(center * center, axis=-1, keepdims=True)
    return center * lax.rsqrt(variance + EPS) * gain


def gelu(v):
    return 0.5 * v * (1.0 + lax.erf(v * 0.7071067811865476))


def kernel(
    tok_ref, gain_ref, qkv_ref, up_ref, qg_ref, kg_ref, wo_ref, wd_ref, ak_ref, fk_ref,
    out_ref,
    ak, fk, w1, w2a, w2b,
    r0, xg, st, xn, s1, r1, keep, s2, r2,
    seg, asend, att, pa, far0, near0, fin0, pp,
    far1, near1, mid, near2, fin, msg, rout, asem_s, asem_r,
    ssem, rsem, lsem,
):
    yh, c, x, yl, z = (lax.axis_index(a) for a in AXES)
    gx = yh * 2 + c
    zh, zl = z // 2, lax.rem(z, 2)

    def ring(v, off):
        return lax.rem(v + off + 4, 4)

    def flip(v, d):
        return lax.rem(v + d, 2)

    xs = [ring(x, o) for o in (0, -1, 1, 2)]
    zs = [ring(z, o) for o in (0, -1, 1, 2)]
    xp, xm, zp, zm = {"x": xs[2]}, {"x": xs[1]}, {"z": zs[2]}, {"z": zs[1]}
    peers = {
        (0, 1): {"core": 1 - c},
        (1, 0): {"yh": 1 - yh},
        (1, 1): {"yh": 1 - yh, "core": 1 - c},
    }
    same = gx == x

    def partner(dy, dz):
        return {
            "yh": x // 2,
            "core": lax.rem(x, 2),
            "x": gx,
            "yl": flip(yl, dy),
            "z": zh * 2 + flip(zl, dz),
        }

    count = [0]
    started = []

    def send(src, dst, dev, start=True):
        i = count[0]
        count[0] += 1
        copy = pltpu.make_async_remote_copy(
            src_ref=src, dst_ref=dst, send_sem=ssem.at[i], recv_sem=rsem.at[i],
            device_id=dev, device_id_type=MESH,
        )
        if start:
            copy.start()
            started.append(copy)
        return copy

    locals_ = [0]

    def load(src, dst):
        i = locals_[0]
        locals_[0] += 1
        copy = pltpu.make_async_copy(src, dst, lsem.at[i])
        copy.start()
        return copy

    loads1, loads2, loads4 = [], [], []
    for t in range(4):
        a, b = t // 2, t % 2
        nat = (b * 2 + a) * 384
        for k in range(3):
            loads1.append(load(qkv_ref.at[k, pl.ds(nat, 384)], w1.at[a, pl.ds(b * 384, 384), pl.ds(k * 128, 128)]))
        loads1.append(load(up_ref.at[pl.ds(nat, 384)], w1.at[a, pl.ds(b * 384, 384), pl.ds(384, 768)]))
    for t in range(4):
        a, b = t // 2, t % 2
        nat = (b * 2 + a) * 384
        loads4.append(load(wo_ref.at[:, pl.ds(nat, 384)], w2a.at[x, :, pl.ds(t * 384, 384)]))
        loads2.append(load(wd_ref.at[:, pl.ds(nat, 384)], w2b.at[:, pl.ds(t * 384, 384)]))
    loads3 = [load(ak_ref, ak), load(fk_ref, fk)]

    barrier = pltpu.get_barrier_semaphore()

    def greet(dev):
        pl.semaphore_signal(barrier, inc=1, device_id=dev, device_id_type=MESH)

    for dev in (xp, xm, {"x": xs[3]}, zp, zm, {"z": zs[3]}, *peers.values()):
        greet(dev)
    for dy, dz in ((0, 0), (0, 1), (1, 0), (1, 1)):
        greet(partner(dy, dz))
    for k in range(4):
        greet({"yh": x // 2, "core": lax.rem(x, 2), "x": k})
    pl.semaphore_wait(barrier, 17)

    def lanes(h):
        return pl.ds(pl.multiple_of(h * 128, 128), 128)

    first = {}
    for dy, dz in ((0, 0), (0, 1), (1, 0), (1, 1)):
        whole = dy + dz == 0
        copy = send(tok_ref.at[:, lanes(flip(zl, dz))], r0.at[yl, zl], partner(dy, dz), start=not whole)
        first[dy, dz] = copy
        if whole:
            mine = pltpu.make_async_copy(tok_ref.at[:, lanes(zl)], r0.at[yl, zl], lsem.at[N_LOCAL - 1])

            @pl.when(same)
            def _():
                mine.start()
                mine.wait()

            @pl.when(jnp.logical_not(same))
            def _():
                copy.start()

    @pl.when(jnp.logical_not(same))
    def _():
        first[0, 0].wait()

    for key in ((0, 1), (1, 0), (1, 1)):
        first[key].wait_recv()

    arrived = r0[...].reshape(768, 128).T
    for r in range(4):
        lo = (r // 2) * 32
        xg[r % 2, x, zh, zl, lo : lo + 32] = arrived[r * 32 : (r + 1) * 32]

    def gather(g):
        def push(ref, dev):
            return send(ref, ref, dev)

        def piece(img, zz, lo):
            return xg.at[g, img, zz // 2, lax.rem(zz, 2), pl.ds(lo, 32)]

        def by_z(k, zz):
            return xg.at[g, pl.ds(k * 2, 2), zz // 2, lax.rem(zz, 2), pl.ds(0, 32)]

        def by_x(k, img):
            return xg.at[g, img, k, :, pl.ds(32, 32)]

        near = [push(piece(x, z, 0), d) for d in (xp, xm, {"x": xs[3]})]
        near += [push(piece(x, z, 32), d) for d in (zp, zm, {"z": zs[3]})]
        yield
        for copy in near:
            copy.wait_recv()
        up = [(push(by_z(k, z), zp), push(by_x(k, x), xp)) for k in (0, 1)]
        down = [(push(by_z(k, z), zm), push(by_x(k, x), xm)) for k in (1, 0)]
        yield
        rest = []
        up[0][0].wait_recv()
        rest.append(push(by_z(0, zs[1]), zp))
        up[0][1].wait_recv()
        rest.append(push(by_x(0, xs[1]), xp))
        down[0][0].wait_recv()
        rest.append(push(by_z(1, zs[2]), zm))
        down[0][1].wait_recv()
        rest.append(push(by_x(1, xs[2]), xm))
        yield
        for copy in (*up[1], *down[1], *rest):
            copy.wait_recv()
        yield

    eye = lax.broadcasted_iota(jnp.int32, (128, 128), 0) == lax.broadcasted_iota(jnp.int32, (128, 128), 1)

    def to_row(col):
        return jnp.sum(jnp.where(eye, jnp.broadcast_to(col, (128, 128)), 0.0), axis=0, keepdims=True)

    def to_col(row):
        return jnp.sum(jnp.where(eye, jnp.broadcast_to(row, (128, 128)), 0.0), axis=1, keepdims=True)

    def statistics(g):
        @pl.loop(0, 4)
        def _(m):
            lo = xg[g, m, 0].reshape(128, 768).astype(F32)
            hi = xg[g, m, 1].reshape(128, 768).astype(F32)
            mean = (jnp.sum(lo, axis=1, keepdims=True) + jnp.sum(hi, axis=1, keepdims=True)) * (1.0 / 1536.0)
            dl, dh = lo - mean, hi - mean
            spread = jnp.sum(dl * dl, axis=1, keepdims=True) + jnp.sum(dh * dh, axis=1, keepdims=True)
            st[0, g, m, 0:1] = to_row(mean)
            st[0, g, m, 1:2] = to_row(spread)

        return [send(st.at[0, g], st.at[d[0] * 2 + d[1], g], peers[d]) for d in peers]

    def far_img(dyh, dc):
        return flip(yh, dyh) * 2 + flip(c, dc)

    def normalise(g):
        for i, (dyh, dc) in enumerate(((1, 1), (0, 1), (1, 0), (0, 0))):
            m = far_img(dyh, dc)
            means = [st[k, g, m, 0:1] for k in range(4)]
            mean = (means[0] + means[1] + means[2] + means[3]) * 0.25
            spread = sum(st[k, g, m, 1:2] + 1536.0 * (means[k] - mean) * (means[k] - mean) for k in range(4))
            scale = lax.rsqrt(spread * (1.0 / 6144.0) + EPS)
            mean_c, scale_c = to_col(mean), to_col(scale)
            for a in range(2):
                for b in range(2):
                    gain = gain_ref[gx, 0:1, (b * 2 + a) * 384 : (b * 2 + a + 1) * 384]
                    cols = slice(b * 384, (b + 1) * 384)
                    v = xg[g, m, a, :, :, cols].reshape(128, 384).astype(F32)
                    xn[a, i * 128 : (i + 1) * 128, cols] = ((v - mean_c) * scale_c * gain).astype(BF)

    core_copy, y_copy = {}, {}

    def first_matmul(g, n):
        cols = slice(n * 384, (n + 1) * 384)
        y = jnp.dot(xn[0], w1[0, :, cols], preferred_element_type=F32)
        y = y + jnp.dot(xn[1], w1[1, :, cols], preferred_element_type=F32)
        s1[g, n] = y[0:256].astype(BF).reshape(2, 128, 384)
        core_copy[g, n] = send(s1.at[g, n], r1.at[g, n], peers[0, 1])
        keep[g, n] = y[256:512].reshape(2, 128, 384)

    def pass_on(g, n):
        core_copy[g, n].wait_recv()
        s2[g, n] = (keep[g, n, 0] + r1[g, n, 0].astype(F32)).astype(BF)
        y_copy[g, n] = send(s2.at[g, n], r2.at[g, n], peers[1, 0])

    def united(g, n):
        y_copy[g, n].wait_recv()
        return keep[g, n, 1] + r1[g, n, 1].astype(F32) + r2[g, n].astype(F32)

    spread_y, spread_c, forwards = {}, {}, {}

    def seg_at(g, n, m):
        return seg.at[g, m, :, :, pl.ds((n - 1) * 384, 384)]

    def hidden(g, n):
        v = gelu(united(g, n)).astype(BF)
        seg[g, gx, :, :, (n - 1) * 384 : n * 384] = v.reshape(2, 64, 384)
        spread_y[g, n] = send(seg_at(g, n, gx), seg_at(g, n, gx), peers[1, 0])
        spread_c[g, n] = send(seg_at(g, n, gx), seg_at(g, n, gx), peers[0, 1])

    def forward(g, n):
        spread_y[g, n].wait_recv()
        m = far_img(1, 0)
        forwards[g, n] = send(seg_at(g, n, m), seg_at(g, n, m), peers[0, 1])

    def to_row_owner(dyh, dc):
        i = dyh * 2 + dc
        dev = {"yh": flip(yh, dyh), "core": flip(c, dc), "x": gx}
        return pltpu.make_async_remote_copy(
            src_ref=asend, dst_ref=att.at[x], send_sem=asem_s.at[i], recv_sem=asem_r.at[x],
            device_id=dev, device_id_type=MESH,
        )

    def attention():
        mine = jnp.concatenate([united(0, 0), united(1, 0)], axis=0)
        queries = norm_rows(mine[:, 0:128], qg_ref[...]).astype(BF)
        keys = norm_rows(mine[:, 128:256], kg_ref[...]).astype(BF)
        values = mine[:, 256:384].astype(BF)
        scores = lax.dot_general(queries, keys, (((1,), (1,)), ((), ())), preferred_element_type=F32) * (128 ** -0.5)
        raised = jnp.exp(scores)
        weights = (raised / jnp.sum(raised, axis=-1, keepdims=True)).astype(BF)
        asend[...] = jnp.dot(weights, values, preferred_element_type=F32).astype(BF)

        @pl.when(same)
        def _():
            pltpu.make_async_copy(asend, att.at[x], asem_r.at[x]).start()

        @pl.when(jnp.logical_not(same))
        def _():
            to_row_owner(0, 0).start()

        for d in peers:
            to_row_owner(*d).start()

    for copy in loads4:
        copy.wait()

    def ring_rs(part, devp, devm, dest, far, near, out):
        f0 = send(part(0, dest[3]), far.at[0], devp)
        f1 = send(part(1, dest[3]), far.at[1], devm)
        o1 = send(part(1, dest[2]), near.at[0, 1], devp)
        o0 = send(part(0, dest[1]), near.at[1, 0], devm)
        late = []

        def middle():
            f0.wait_recv()
            ref = part(0, dest[2])
            ref[...] = (ref[...].astype(F32) + far[0].astype(F32)).astype(BF)
            late.append(send(ref, near.at[0, 0], devp))
            f1.wait_recv()
            ref = part(1, dest[1])
            ref[...] = (ref[...].astype(F32) + far[1].astype(F32)).astype(BF)
            late.append(send(ref, near.at[1, 1], devm))

        def end():
            for copy in (o1, o0, *late):
                copy.wait_recv()
            for br in range(2):
                total = part(br, dest[0])[...].astype(F32) + near[0, br].astype(F32) + near[1, br].astype(F32)
                out[br] = total.astype(BF)

        return middle, end

    def attended_matmul():
        for k in range(4):
            pltpu.make_async_remote_copy(
                src_ref=asend, dst_ref=att.at[k], send_sem=asem_s.at[0], recv_sem=asem_r.at[k],
                device_id=peers[0, 1], device_id_type=MESH,
            ).wait_recv()
        for copy in wo2:
            copy.wait_recv()
        left = jnp.concatenate([att[k] for k in range(4)], axis=1)
        for a in range(2):
            right = w2a[:, :, a * 768 : (a + 1) * 768].reshape(512, 768)
            y = jnp.dot(left, right, preferred_element_type=F32).astype(BF)
            for g in range(2):
                pa[a, :, g] = y[g * 128 : (g + 1) * 128].reshape(2, 64, 768)

    def second_matmul(g):
        for n in (1, 2):
            spread_c[g, n].wait_recv()
            forwards[g, n].wait_recv()
        for a in range(2):
            y = jnp.dot(seg[g].reshape(512, 768), w2b[:, a * 768 : (a + 1) * 768], preferred_element_type=F32)
            pp[g, a] = y.astype(BF).reshape(4, 2, 64, 768)

    def stage0():
        part = lambda k, d: pa.at[d // 2, lax.rem(d, 2), k]
        return ring_rs(part, zp, zm, zs, far0, near0, fin0)

    def stage1(r):
        g = r % 2
        if r < 2:
            part = lambda k, d: pp.at[g, d // 2, pl.ds(k * 2, 2), lax.rem(d, 2), pl.ds(0, 32)]
            return ring_rs(part, zp, zm, zs, far1.at[r], near1.at[r], mid.at[r])
        part = lambda k, d: pp.at[g, k, d, :, pl.ds(32, 32)]
        return ring_rs(part, xp, xm, xs, far1.at[r], near1.at[r], mid.at[r])

    def stage2(r):
        dests, devs = (xs, (xm, xp, {"x": xs[3]})) if r < 2 else (zs, (zm, zp, {"z": zs[3]}))
        at = lambda d: mid.at[r, d // 2, lax.rem(d, 2)]
        copies = [send(at(dests[k + 1]), near2.at[r, k], devs[k]) for k in range(3)]

        def end():
            for copy in copies:
                copy.wait_recv()
            total = at(dests[0])[...].astype(F32)
            for k in range(3):
                total = total + near2[r, k].astype(F32)
            fin[r] = total.astype(BF)

        return end

    home = {}

    def deliver(r):
        for q in range(4):
            cols = slice(q * 192, (q + 1) * 192)
            msg[r, q] = jnp.concatenate([fin0[r % 2, (r // 2) * 32 : (r // 2) * 32 + 32, cols], fin[r, :, cols]], axis=1)
        for dy, dz in ((0, 0), (0, 1), (1, 0), (1, 1)):
            whole = dy + dz == 0
            q = flip(yl, dy) * 2 + flip(zl, dz)
            copy = send(msg.at[r, q], rout.at[yl, zl, r], partner(dy, dz), start=not whole)
            home[r, dy, dz] = copy
            if whole:
                @pl.when(same)
                def _():
                    rout[yl, zl, r] = msg[r, q]

                @pl.when(jnp.logical_not(same))
                def _():
                    copy.start()

    mids, ends, ends2 = {}, {}, {}

    def begin(r):
        mids[r], ends[r] = stage1(r)

    def turn(r):
        ends[r]()
        ends2[r] = stage2(r)

    def close(r):
        ends2[r]()
        deliver(r)

    ag0, ag1 = gather(0), gather(1)
    next(ag0)
    next(ag1)
    next(ag0)
    next(ag0)
    next(ag1)
    next(ag0)
    shared0 = statistics(0)
    next(ag1)
    for copy in shared0:
        copy.wait_recv()
    for copy in loads1:
        copy.wait()
    normalise(0)
    first_matmul(0, 0)
    first_matmul(0, 1)
    pass_on(0, 0)
    next(ag1)
    shared1 = statistics(1)
    first_matmul(0, 2)
    pass_on(0, 1)
    wo1 = (send(w2a.at[x], w2a.at[x], xp), send(w2a.at[x], w2a.at[x], xm))
    for copy in shared1:
        copy.wait_recv()
    pass_on(0, 2)
    normalise(1)
    first_matmul(1, 0)
    hidden(0, 1)
    first_matmul(1, 1)
    pass_on(1, 0)
    first_matmul(1, 2)
    hidden(0, 2)
    pass_on(1, 1)
    pass_on(1, 2)
    wo1[0].wait_recv()
    wo2 = [send(w2a.at[xs[1], pl.ds(0, 64)], w2a.at[xs[1], pl.ds(0, 64)], xp)]
    wo1[1].wait_recv()
    wo2.append(send(w2a.at[xs[2], pl.ds(64, 64)], w2a.at[xs[2], pl.ds(64, 64)], xm))
    forward(0, 1)
    attention()
    forward(0, 2)
    hidden(1, 1)
    for copy in loads2:
        copy.wait()
    second_matmul(0)
    begin(0)
    begin(2)
    hidden(1, 2)
    forward(1, 1)
    attended_matmul()
    mid0, end0 = stage0()
    mids[0]()
    mids[2]()
    forward(1, 2)
    second_matmul(1)
    begin(1)
    begin(3)
    mid0()
    turn(0)
    turn(2)
    end0()
    mids[1]()
    mids[3]()
    close(0)
    close(2)
    turn(1)
    turn(3)
    close(1)
    close(3)

    for copy in loads3:
        copy.wait()
    for r in range(4):
        for dy, dz in ((0, 1), (1, 0), (1, 1)):
            home[r, dy, dz].wait_recv()

        @pl.when(jnp.logical_not(same))
        def _():
            home[r, 0, 0].wait()

    for h in range(2):
        total = (rout[0, h].astype(F32) + rout[1, h].astype(F32)).reshape(128, 384).T
        cols = slice(h * 128, (h + 1) * 128)
        branches = ak[:, cols].astype(F32) * total[0:192] + fk[:, cols].astype(F32) * total[192:384]
        out_ref[:, cols] = (tok_ref[:, cols].astype(F32) + branches * KEEP_SCALE).astype(BF)

    @pl.when(jnp.logical_not(same))
    def _():
        to_row_owner(0, 0).wait_send()

    for d in peers:
        to_row_owner(*d).wait_send()
    for copy in started:
        copy.wait_send()


def per_device(tokens, norm_gain, qkv_weight, up_weight, query_gain, key_gain, out_weight, down_weight, ak, fk):
    vm = pl.BlockSpec(memory_space=pltpu.VMEM)
    hbm = pl.BlockSpec(memory_space=pl.ANY)
    V = pltpu.VMEM
    scratch = [
        V((192, 256), jnp.int32), V((192, 256), jnp.int32),
        V((2, 768, 1152), BF), V((4, 128, 1536), BF), V((768, 1536), BF),
        V((2, 2, 192, 128), BF), V((2, 4, 2, 2, 64, 768), BF), V((4, 2, 4, 8, 128), F32), V((2, 512, 768), BF),
        V((2, 3, 2, 128, 384), BF), V((2, 3, 2, 128, 384), BF), V((2, 3, 2, 128, 384), F32),
        V((2, 3, 128, 384), BF), V((2, 3, 128, 384), BF),
        V((2, 4, 2, 64, 768), BF), V((256, 128), BF), V((4, 256, 128), BF),
        V((2, 2, 2, 64, 768), BF), V((2, 64, 768), BF), V((2, 2, 64, 768), BF), V((2, 64, 768), BF),
        V((2, 2, 4, 2, 64, 768), BF),
        V((4, 2, 2, 32, 768), BF), V((4, 2, 2, 2, 32, 768), BF), V((4, 2, 2, 32, 768), BF),
        V((4, 3, 32, 768), BF), V((4, 32, 768), BF),
        V((4, 4, 32, 384), BF), V((2, 2, 4, 32, 384), BF),
        pltpu.SemaphoreType.DMA((4,)), pltpu.SemaphoreType.DMA((4,)),
        pltpu.SemaphoreType.DMA((N_COPIES,)), pltpu.SemaphoreType.DMA((N_COPIES,)), pltpu.SemaphoreType.DMA((N_LOCAL,)),
    ]
    out = pl.pallas_call(
        kernel,
        out_shape=jax.ShapeDtypeStruct((192, 256), BF),
        in_specs=[vm, vm, hbm, hbm, vm, vm, hbm, hbm, hbm, hbm],
        out_specs=vm,
        scratch_shapes=scratch,
        compiler_params=pltpu.CompilerParams(collective_id=0, has_side_effects=True, vmem_limit_bytes=60000 * 1024),
        name="block",
    )(
        tokens[0].T,
        norm_gain.reshape(4, 1, 1536),
        qkv_weight.transpose(1, 0, 2),
        up_weight,
        query_gain.reshape(1, 128),
        key_gain.reshape(1, 128),
        out_weight,
        down_weight,
        ak[0].T,
        fk[0].T,
    )
    return out.T[None]


def solution(mesh):
    split = Mesh(mesh.devices.reshape(2, 2, 4, 2, 4), AXES)
    gx, gy = ("yh", "core"), ("x", "yl", "z")
    placed = (
        P(gx, None, gy), P(), P(gx, None, gy), P(gx, gy), P(), P(), P(gy, gx), P(gy, gx), P(gx, None, gy), P(gx, None, gy),
    )
    return jax.shard_map(per_device, mesh=split, in_specs=placed, out_specs=P(gx, None, gy), check_vma=False)
```

```python
import jax
import jax.numpy as jnp
from jax import lax
from jax.experimental import pallas as pl
from jax.experimental.pallas import tpu as pltpu
from jax.sharding import Mesh
from jax.sharding import PartitionSpec as P

MESH = pl.DeviceIdType.MESH
AXES = ("yh", "core", "x", "yl", "z")
EPS = 1e-06
KEEP_SCALE = 1.0 / 0.9
BF = jnp.bfloat16
F32 = jnp.float32
N_COPIES = 132
N_SENDS = 32
N_LOCAL = 6


def norm_rows(values, gain):
    center = values - jnp.mean(values, axis=-1, keepdims=True)
    variance = jnp.mean(center * center, axis=-1, keepdims=True)
    return center * lax.rsqrt(variance + EPS) * gain


def gelu(v):
    return 0.5 * v * (1.0 + lax.erf(v * 0.7071067811865476))


def kernel(
    tok_ref, gain_ref, qkv_ref, up_ref, qg_ref, kg_ref, wo_ref, wd_ref, ak_ref, fk_ref,
    out_ref,
    ak, fk, w1, w2a, w2b,
    r0, xg, st, xn, s1, r1, keep, s2, r2,
    seg, asend, att, pa, far0, near0, fin0, pp,
    far1, near1, mid, near2, fin, msg, rout, asem_s, asem_r,
    ssem, rsem, lsem,
):
    yh, c, x, yl, z = (lax.axis_index(a) for a in AXES)
    gx = yh * 2 + c
    zh, zl = z // 2, lax.rem(z, 2)

    def ring(v, off):
        return lax.rem(v + off + 4, 4)

    def flip(v, d):
        return lax.rem(v + d, 2)

    xs = [ring(x, o) for o in (0, -1, 1, 2)]
    zs = [ring(z, o) for o in (0, -1, 1, 2)]
    xp, xm, zp, zm = {"x": xs[2]}, {"x": xs[1]}, {"z": zs[2]}, {"z": zs[1]}
    peers = {
        (0, 1): {"core": 1 - c},
        (1, 0): {"yh": 1 - yh},
        (1, 1): {"yh": 1 - yh, "core": 1 - c},
    }
    same = gx == x

    def partner(dy, dz):
        return {
            "yh": x // 2,
            "core": lax.rem(x, 2),
            "x": gx,
            "yl": flip(yl, dy),
            "z": zh * 2 + flip(zl, dz),
        }

    count = [0]
    sending = {}

    def finish(entry):
        copy, always = entry
        if always:
            copy.wait_send()
        else:
            @pl.when(jnp.logical_not(same))
            def _():
                copy.wait_send()


    def send(src, dst, dev, start=True):
        i = count[0]
        count[0] += 1
        j = i % N_SENDS
        copy = pltpu.make_async_remote_copy(
            src_ref=src, dst_ref=dst, send_sem=ssem.at[j], recv_sem=rsem.at[i],
            device_id=dev, device_id_type=MESH,
        )
        if j in sending:
            finish(sending.pop(j))
        sending[j] = copy, start
        if start:
            copy.start()
        return copy

    locals_ = [0]

    def load(src, dst):
        copy = pltpu.make_async_copy(src, dst, lsem.at[locals_[0]])
        copy.start()
        return copy

    def all_of(ref):
        copy = pltpu.make_async_copy(ref, ref, lsem.at[locals_[0]])
        locals_[0] += 1
        return [copy]

    for t in range(4):
        a, b = t // 2, t % 2
        nat = (b * 2 + a) * 384
        for k in range(3):
            load(qkv_ref.at[k, pl.ds(nat, 384)], w1.at[a, pl.ds(b * 384, 384), pl.ds(k * 128, 128)])
        load(up_ref.at[pl.ds(nat, 384)], w1.at[a, pl.ds(b * 384, 384), pl.ds(384, 768)])
    loads1 = all_of(w1)
    for t in range(4):
        nat = ((t % 2) * 2 + t // 2) * 384
        load(wo_ref.at[:, pl.ds(nat, 384)], w2a.at[x, :, pl.ds(t * 384, 384)])
    loads4 = all_of(w2a.at[x])
    for t in range(4):
        nat = ((t % 2) * 2 + t // 2) * 384
        load(wd_ref.at[:, pl.ds(nat, 384)], w2b.at[:, pl.ds(t * 384, 384)])
    loads2 = all_of(w2b)
    load(ak_ref, ak)
    loads3 = all_of(ak)
    load(fk_ref, fk)
    loads3 += all_of(fk)

    barrier = pltpu.get_barrier_semaphore()

    def greet(dev):
        pl.semaphore_signal(barrier, inc=1, device_id=dev, device_id_type=MESH)

    for dev in (xp, xm, {"x": xs[3]}, zp, zm, {"z": zs[3]}, *peers.values()):
        greet(dev)
    for dy, dz in ((0, 0), (0, 1), (1, 0), (1, 1)):
        greet(partner(dy, dz))
    for k in range(4):
        greet({"yh": x // 2, "core": lax.rem(x, 2), "x": k})
    pl.semaphore_wait(barrier, 17)

    def lanes(h):
        return pl.ds(pl.multiple_of(h * 128, 128), 128)

    first = {}
    for dy, dz in ((0, 0), (0, 1), (1, 0), (1, 1)):
        whole = dy + dz == 0
        copy = send(tok_ref.at[:, lanes(flip(zl, dz))], r0.at[yl, zl], partner(dy, dz), start=not whole)
        first[dy, dz] = copy
        if whole:
            mine = pltpu.make_async_copy(tok_ref.at[:, lanes(zl)], r0.at[yl, zl], lsem.at[N_LOCAL - 1])

            @pl.when(same)
            def _():
                mine.start()
                mine.wait()

            @pl.when(jnp.logical_not(same))
            def _():
                copy.start()

    @pl.when(jnp.logical_not(same))
    def _():
        first[0, 0].wait_recv()

    for key in ((0, 1), (1, 0), (1, 1)):
        first[key].wait_recv()

    arrived = r0[...].reshape(768, 128).T
    for r in range(4):
        lo = (r // 2) * 32
        xg[r % 2, x, zh, zl, lo : lo + 32] = arrived[r * 32 : (r + 1) * 32]

    def gather(g):
        def push(ref, dev):
            return send(ref, ref, dev)

        def piece(img, zz, lo):
            return xg.at[g, img, zz // 2, lax.rem(zz, 2), pl.ds(lo, 32)]

        def by_z(k, zz):
            return xg.at[g, pl.ds(k * 2, 2), zz // 2, lax.rem(zz, 2), pl.ds(0, 32)]

        def by_x(k, img):
            return xg.at[g, img, k, :, pl.ds(32, 32)]

        near = [push(piece(x, z, 0), d) for d in (xp, xm, {"x": xs[3]})]
        near += [push(piece(x, z, 32), d) for d in (zp, zm, {"z": zs[3]})]
        yield
        for copy in near:
            copy.wait_recv()
        up = [(push(by_z(k, z), zp), push(by_x(k, x), xp)) for k in (0, 1)]
        down = [(push(by_z(k, z), zm), push(by_x(k, x), xm)) for k in (1, 0)]
        yield
        rest = []
        up[0][0].wait_recv()
        rest.append(push(by_z(0, zs[1]), zp))
        up[0][1].wait_recv()
        rest.append(push(by_x(0, xs[1]), xp))
        down[0][0].wait_recv()
        rest.append(push(by_z(1, zs[2]), zm))
        down[0][1].wait_recv()
        rest.append(push(by_x(1, xs[2]), xm))
        yield
        for copy in (*up[1], *down[1], *rest):
            copy.wait_recv()
        yield

    eye = lax.broadcasted_iota(jnp.int32, (128, 128), 0) == lax.broadcasted_iota(jnp.int32, (128, 128), 1)

    def to_row(col):
        return jnp.sum(jnp.where(eye, jnp.broadcast_to(col, (128, 128)), 0.0), axis=0, keepdims=True)

    def to_col(row):
        return jnp.sum(jnp.where(eye, jnp.broadcast_to(row, (128, 128)), 0.0), axis=1, keepdims=True)

    def statistics(g):
        @pl.loop(0, 4)
        def _(m):
            lo = xg[g, m, 0].reshape(128, 768).astype(F32)
            hi = xg[g, m, 1].reshape(128, 768).astype(F32)
            mean = (jnp.sum(lo, axis=1, keepdims=True) + jnp.sum(hi, axis=1, keepdims=True)) * (1.0 / 1536.0)
            dl, dh = lo - mean, hi - mean
            spread = jnp.sum(dl * dl, axis=1, keepdims=True) + jnp.sum(dh * dh, axis=1, keepdims=True)
            st[0, g, m, 0:1] = to_row(mean)
            st[0, g, m, 1:2] = to_row(spread)

        return [send(st.at[0, g], st.at[d[0] * 2 + d[1], g], peers[d]) for d in peers]

    def far_img(dyh, dc):
        return flip(yh, dyh) * 2 + flip(c, dc)

    def normalise(g):
        for i, (dyh, dc) in enumerate(((1, 1), (0, 1), (1, 0), (0, 0))):
            m = far_img(dyh, dc)
            means = [st[k, g, m, 0:1] for k in range(4)]
            mean = (means[0] + means[1] + means[2] + means[3]) * 0.25
            spread = sum(st[k, g, m, 1:2] + 1536.0 * (means[k] - mean) * (means[k] - mean) for k in range(4))
            scale = lax.rsqrt(spread * (1.0 / 6144.0) + EPS)
            mean_c, scale_c = to_col(mean), to_col(scale)
            for a in range(2):
                for b in range(2):
                    gain = gain_ref[gx, 0:1, (b * 2 + a) * 384 : (b * 2 + a + 1) * 384]
                    cols = slice(b * 384, (b + 1) * 384)
                    v = xg[g, m, a, :, :, cols].reshape(128, 384).astype(F32)
                    xn[a, i * 128 : (i + 1) * 128, cols] = ((v - mean_c) * scale_c * gain).astype(BF)

    core_copy, y_copy = {}, {}

    def first_matmul(g, n):
        cols = slice(n * 384, (n + 1) * 384)
        y = jnp.dot(xn[0], w1[0, :, cols], preferred_element_type=F32)
        y = y + jnp.dot(xn[1], w1[1, :, cols], preferred_element_type=F32)
        s1[g, n] = y[0:256].astype(BF).reshape(2, 128, 384)
        core_copy[g, n] = send(s1.at[g, n], r1.at[g, n], peers[0, 1])
        keep[g, n] = y[256:512].reshape(2, 128, 384)

    def pass_on(g, n):
        core_copy[g, n].wait_recv()
        s2[g, n] = (keep[g, n, 0] + r1[g, n, 0].astype(F32)).astype(BF)
        y_copy[g, n] = send(s2.at[g, n], r2.at[g, n], peers[1, 0])

    def united(g, n):
        y_copy[g, n].wait_recv()
        return keep[g, n, 1] + r1[g, n, 1].astype(F32) + r2[g, n].astype(F32)

    spread_y, spread_c, forwards = {}, {}, {}

    def seg_at(g, n, m):
        return seg.at[g, m, :, :, pl.ds((n - 1) * 384, 384)]

    def hidden(g, n):
        v = gelu(united(g, n)).astype(BF)
        seg[g, gx, :, :, (n - 1) * 384 : n * 384] = v.reshape(2, 64, 384)
        spread_y[g, n] = send(seg_at(g, n, gx), seg_at(g, n, gx), peers[1, 0])
        spread_c[g, n] = send(seg_at(g, n, gx), seg_at(g, n, gx), peers[0, 1])

    def forward(g, n):
        spread_y[g, n].wait_recv()
        m = far_img(1, 0)
        forwards[g, n] = send(seg_at(g, n, m), seg_at(g, n, m), peers[0, 1])

    def to_row_owner(dyh, dc):
        i = dyh * 2 + dc
        dev = {"yh": flip(yh, dyh), "core": flip(c, dc), "x": gx}
        return pltpu.make_async_remote_copy(
            src_ref=asend, dst_ref=att.at[x], send_sem=asem_s.at[i], recv_sem=asem_r.at[x],
            device_id=dev, device_id_type=MESH,
        )

    def attention():
        mine = jnp.concatenate([united(0, 0), united(1, 0)], axis=0)
        queries = norm_rows(mine[:, 0:128], qg_ref[...]).astype(BF)
        keys = norm_rows(mine[:, 128:256], kg_ref[...]).astype(BF)
        values = mine[:, 256:384].astype(BF)
        scores = lax.dot_general(queries, keys, (((1,), (1,)), ((), ())), preferred_element_type=F32) * (128 ** -0.5)
        raised = jnp.exp(scores)
        weights = (raised / jnp.sum(raised, axis=-1, keepdims=True)).astype(BF)
        asend[...] = jnp.dot(weights, values, preferred_element_type=F32).astype(BF)

        @pl.when(same)
        def _():
            pltpu.make_async_copy(asend, att.at[x], asem_r.at[x]).start()

        @pl.when(jnp.logical_not(same))
        def _():
            to_row_owner(0, 0).start()

        for d in peers:
            to_row_owner(*d).start()

    for copy in loads4:
        copy.wait()

    def ring_rs(part, devp, devm, dest, far, near, out):
        f0 = send(part(0, dest[3]), far.at[0], devp)
        f1 = send(part(1, dest[3]), far.at[1], devm)
        o1 = send(part(1, dest[2]), near.at[0, 1], devp)
        o0 = send(part(0, dest[1]), near.at[1, 0], devm)
        late = []

        def middle():
            f0.wait_recv()
            ref = part(0, dest[2])
            ref[...] = (ref[...].astype(F32) + far[0].astype(F32)).astype(BF)
            late.append(send(ref, near.at[0, 0], devp))
            f1.wait_recv()
            ref = part(1, dest[1])
            ref[...] = (ref[...].astype(F32) + far[1].astype(F32)).astype(BF)
            late.append(send(ref, near.at[1, 1], devm))

        def end():
            for copy in (o1, o0, *late):
                copy.wait_recv()
            for br in range(2):
                total = part(br, dest[0])[...].astype(F32) + near[0, br].astype(F32) + near[1, br].astype(F32)
                out[br] = total.astype(BF)

        return middle, end

    def attended_matmul():
        for k in range(4):
            pltpu.make_async_remote_copy(
                src_ref=asend, dst_ref=att.at[k], send_sem=asem_s.at[0], recv_sem=asem_r.at[k],
                device_id=peers[0, 1], device_id_type=MESH,
            ).wait_recv()
        for copy in wo2:
            copy.wait_recv()
        left = jnp.concatenate([att[k] for k in range(4)], axis=1)
        for a in range(2):
            right = w2a[:, :, a * 768 : (a + 1) * 768].reshape(512, 768)
            y = jnp.dot(left, right, preferred_element_type=F32).astype(BF)
            for g in range(2):
                pa[a, :, g] = y[g * 128 : (g + 1) * 128].reshape(2, 64, 768)

    def second_matmul(g):
        for n in (1, 2):
            spread_c[g, n].wait_recv()
            forwards[g, n].wait_recv()
        for a in range(2):
            y = jnp.dot(seg[g].reshape(512, 768), w2b[:, a * 768 : (a + 1) * 768], preferred_element_type=F32)
            pp[g, a] = y.astype(BF).reshape(4, 2, 64, 768)

    def stage0():
        part = lambda k, d: pa.at[d // 2, lax.rem(d, 2), k]
        return ring_rs(part, zp, zm, zs, far0, near0, fin0)

    def stage1(r):
        g = r % 2
        if r < 2:
            part = lambda k, d: pp.at[g, d // 2, pl.ds(k * 2, 2), lax.rem(d, 2), pl.ds(0, 32)]
            return ring_rs(part, zp, zm, zs, far1.at[r], near1.at[r], mid.at[r])
        part = lambda k, d: pp.at[g, k, d, :, pl.ds(32, 32)]
        return ring_rs(part, xp, xm, xs, far1.at[r], near1.at[r], mid.at[r])

    def stage2(r):
        dests, devs = (xs, (xm, xp, {"x": xs[3]})) if r < 2 else (zs, (zm, zp, {"z": zs[3]}))
        at = lambda d: mid.at[r, d // 2, lax.rem(d, 2)]
        copies = [send(at(dests[k + 1]), near2.at[r, k], devs[k]) for k in range(3)]

        def end():
            for copy in copies:
                copy.wait_recv()
            total = at(dests[0])[...].astype(F32)
            for k in range(3):
                total = total + near2[r, k].astype(F32)
            fin[r] = total.astype(BF)

        return end

    home = {}

    def deliver(r):
        for q in range(4):
            cols = slice(q * 192, (q + 1) * 192)
            msg[r, q] = jnp.concatenate([fin0[r % 2, (r // 2) * 32 : (r // 2) * 32 + 32, cols], fin[r, :, cols]], axis=1)
        for dy, dz in ((0, 0), (0, 1), (1, 0), (1, 1)):
            whole = dy + dz == 0
            q = flip(yl, dy) * 2 + flip(zl, dz)
            copy = send(msg.at[r, q], rout.at[yl, zl, r], partner(dy, dz), start=not whole)
            home[r, dy, dz] = copy
            if whole:
                @pl.when(same)
                def _():
                    rout[yl, zl, r] = msg[r, q]

                @pl.when(jnp.logical_not(same))
                def _():
                    copy.start()

    mids, ends, ends2 = {}, {}, {}

    def begin(r):
        mids[r], ends[r] = stage1(r)

    def turn(r):
        ends[r]()
        ends2[r] = stage2(r)

    def close(r):
        ends2[r]()
        deliver(r)

    ag0, ag1 = gather(0), gather(1)
    next(ag0)
    next(ag1)
    next(ag0)
    next(ag0)
    next(ag1)
    next(ag0)
    shared0 = statistics(0)
    next(ag1)
    for copy in shared0:
        copy.wait_recv()
    for copy in loads1:
        copy.wait()
    normalise(0)
    first_matmul(0, 0)
    first_matmul(0, 1)
    pass_on(0, 0)
    next(ag1)
    shared1 = statistics(1)
    first_matmul(0, 2)
    pass_on(0, 1)
    wo1 = (send(w2a.at[x], w2a.at[x], xp), send(w2a.at[x], w2a.at[x], xm))
    for copy in shared1:
        copy.wait_recv()
    pass_on(0, 2)
    normalise(1)
    first_matmul(1, 0)
    hidden(0, 1)
    first_matmul(1, 1)
    pass_on(1, 0)
    first_matmul(1, 2)
    hidden(0, 2)
    pass_on(1, 1)
    pass_on(1, 2)
    wo1[0].wait_recv()
    wo2 = [send(w2a.at[xs[1], pl.ds(0, 64)], w2a.at[xs[1], pl.ds(0, 64)], xp)]
    wo1[1].wait_recv()
    wo2.append(send(w2a.at[xs[2], pl.ds(64, 64)], w2a.at[xs[2], pl.ds(64, 64)], xm))
    forward(0, 1)
    attention()
    forward(0, 2)
    for copy in loads2:
        copy.wait()
    second_matmul(0)
    begin(0)
    begin(2)
    hidden(1, 1)
    hidden(1, 2)
    forward(1, 1)
    attended_matmul()
    mid0, end0 = stage0()
    mids[0]()
    mids[2]()
    forward(1, 2)
    second_matmul(1)
    begin(1)
    begin(3)
    mid0()
    turn(0)
    turn(2)
    end0()
    mids[1]()
    mids[3]()
    close(0)
    close(2)
    turn(1)
    turn(3)
    close(1)
    close(3)

    for copy in loads3:
        copy.wait()
    for r in range(4):
        for dy, dz in ((0, 1), (1, 0), (1, 1)):
            home[r, dy, dz].wait_recv()

        @pl.when(jnp.logical_not(same))
        def _():
            home[r, 0, 0].wait_recv()

    for h in range(2):
        total = (rout[0, h].astype(F32) + rout[1, h].astype(F32)).reshape(128, 384).T
        cols = slice(h * 128, (h + 1) * 128)
        branches = ak[:, cols].astype(F32) * total[0:192] + fk[:, cols].astype(F32) * total[192:384]
        out_ref[:, cols] = (tok_ref[:, cols].astype(F32) + branches * KEEP_SCALE).astype(BF)

    @pl.when(jnp.logical_not(same))
    def _():
        to_row_owner(0, 0).wait_send()

    for d in peers:
        to_row_owner(*d).wait_send()
    for entry in sending.values():
        finish(entry)


def per_device(tokens, norm_gain, qkv_weight, up_weight, query_gain, key_gain, out_weight, down_weight, ak, fk):
    vm = pl.BlockSpec(memory_space=pltpu.VMEM)
    hbm = pl.BlockSpec(memory_space=pl.ANY)
    V = pltpu.VMEM
    scratch = [
        V((192, 256), jnp.int32), V((192, 256), jnp.int32),
        V((2, 768, 1152), BF), V((4, 128, 1536), BF), V((768, 1536), BF),
        V((2, 2, 192, 128), BF), V((2, 4, 2, 2, 64, 768), BF), V((4, 2, 4, 8, 128), F32), V((2, 512, 768), BF),
        V((2, 3, 2, 128, 384), BF), V((2, 3, 2, 128, 384), BF), V((2, 3, 2, 128, 384), F32),
        V((2, 3, 128, 384), BF), V((2, 3, 128, 384), BF),
        V((2, 4, 2, 64, 768), BF), V((256, 128), BF), V((4, 256, 128), BF),
        V((2, 2, 2, 64, 768), BF), V((2, 64, 768), BF), V((2, 2, 64, 768), BF), V((2, 64, 768), BF),
        V((2, 2, 4, 2, 64, 768), BF),
        V((4, 2, 2, 32, 768), BF), V((4, 2, 2, 2, 32, 768), BF), V((4, 2, 2, 32, 768), BF),
        V((4, 3, 32, 768), BF), V((4, 32, 768), BF),
        V((4, 4, 32, 384), BF), V((2, 2, 4, 32, 384), BF),
        pltpu.SemaphoreType.DMA((4,)), pltpu.SemaphoreType.DMA((4,)),
        pltpu.SemaphoreType.DMA((N_SENDS,)), pltpu.SemaphoreType.DMA((N_COPIES,)), pltpu.SemaphoreType.DMA((N_LOCAL,)),
    ]
    out = pl.pallas_call(
        kernel,
        out_shape=jax.ShapeDtypeStruct((192, 256), BF),
        in_specs=[vm, vm, hbm, hbm, vm, vm, hbm, hbm, hbm, hbm],
        out_specs=vm,
        scratch_shapes=scratch,
        compiler_params=pltpu.CompilerParams(collective_id=0, has_side_effects=True, vmem_limit_bytes=60000 * 1024),
        name="block",
    )(
        tokens[0].T,
        norm_gain.reshape(4, 1, 1536),
        qkv_weight.transpose(1, 0, 2),
        up_weight,
        query_gain.reshape(1, 128),
        key_gain.reshape(1, 128),
        out_weight,
        down_weight,
        ak[0].T,
        fk[0].T,
    )
    return out.T[None]


def solution(mesh):
    split = Mesh(mesh.devices.reshape(2, 2, 4, 2, 4), AXES)
    gx, gy = ("yh", "core"), ("x", "yl", "z")
    placed = (
        P(gx, None, gy), P(), P(gx, None, gy), P(gx, gy), P(), P(), P(gy, gx), P(gy, gx), P(gx, None, gy), P(gx, None, gy),
    )
    return jax.shard_map(per_device, mesh=split, in_specs=placed, out_specs=P(gx, None, gy), check_vma=False)
```
